256 devices in a mesh: ep: 32 (over x, z), tp: 8 (over y, core).
Axes of the slice: x: 4, y: 4, z: 8, core: 2. Of those that a mesh axis runs over, the one named last changes fastest.
Arguments:
- tokens: bfloat16 [8192, 2880], P('ep', 'tp'), may hold values from -6 to 6
- expert_ids: int32 [8192, 4], P('ep'), may hold values from 0 to 63, all different within a row; in each aligned block of 256 rows (0 to 255, 256 to 511, ...) at most 32 rows name the same one
- combine_weights: float32 [8192, 4], P('ep'), may hold values from 0.05 to 0.6
- gate_weight: bfloat16 [64, 2880, 2880], P('ep', None, 'tp'), may hold values from -0.109375 to 0.109375
- up_weight: bfloat16 [64, 2880, 2880], P('ep', None, 'tp'), may hold values from -0.109375 to 0.109375
- down_weight: bfloat16 [64, 2880, 2880], P('ep', 'tp'), may hold values from -0.109375 to 0.109375
Outputs:
- mixed: bfloat16 [8192, 2880], P('ep', 'tp')
The draws below stay inside these ranges and needn't reach their ends.
Inputs may be any that keep to these rules, and one draw needn't show every extreme that they name: `expert_ids`: each row names 4 different experts; within the 256 rows of one index of ep no expert is named more than 32 times, a bound that some block reaches.
All inputs are finite; a program needn't handle non-finite values.
Results may differ from the reference program's by a relative error of at most 0.014.
Values may be sent and summed in bfloat16 or wider, within the bound.
No kernel may reach another device: no remote copies, remote signals or barrier semaphores. Data moves between devices by JAX's collectives and lax.ppermute only.
A program may use at most 128 MiB of HBM per device.

```python
import math
import jax
import jax.numpy as jnp
import numpy as np
from jax import lax

D = 2880
FF = 2880
TOP = 4
TOK_DEV = 256
EXPERTS = 64
TOKENS = 8192
CAP = 32
FF_DEV = 360
N_EP = 32
N_TP = 8


def shard_levels(stream_key, shape, pieces, smallest, high):
    factor_of = 1.0
    for axis_at, shards_of in pieces:
        heights = jax.random.uniform(jax.random.fold_in(jax.random.fold_in(stream_key, 6), axis_at), (shards_of,), jnp.float32, smallest / len(pieces), high / len(pieces))
        factor_of = factor_of * jnp.repeat(jnp.exp(heights), shape[axis_at] // shards_of).reshape((-1,) + (1,) * (len(shape) - 1 - axis_at))
    return factor_of


def assign_block(key, own, number, rows, count, top, most, skew):
    ranking = jax.random.permutation(key, count)
    packed, usual = portions_of(count, rows * top, most, skew, True), portions_of(count, rows * top, most, skew, False)
    places = jnp.arange(count)

    def named(tallies, offset_by):
        used = int((tallies > 0).sum())
        fixed = max(1, used // 4)
        moved = fixed + (places - fixed + offset_by * (used - fixed)) % max(1, count - fixed)
        return jnp.zeros((count,), jnp.int32).at[ranking[jnp.where(places < fixed, places, moved)]].set(jnp.asarray(tallies, jnp.int32))

    tallies = jnp.where(number % 4 == 0, named(packed, number // 4), named(usual, number - number // 4 - 1))
    mixed = jax.random.permutation(jax.random.fold_in(own, 3), count)
    donor, taker = mixed[0:count // 2 * 2:2], mixed[1:count // 2 * 2:2]
    margin = jnp.minimum(tallies[donor] - 1, most - tallies[taker]) // 2
    margin = jnp.where((donor == ranking[0]) | (taker == ranking[0]) | (tallies[taker] == 0), 0, jnp.maximum(margin, 0))
    moved = jax.random.randint(jax.random.fold_in(own, 4), (count // 2,), 0, 1 << 20) % (margin + 1)
    tallies = tallies.at[donor].add(-moved).at[taker].add(moved)
    labels = jnp.searchsorted(jnp.cumsum(tallies), jnp.arange(rows * top), side="right").astype(jnp.int32)
    table = labels.reshape(top, rows).T
    table = table[jax.random.permutation(jax.random.fold_in(own, 1), rows)]
    offset_by = jax.random.randint(jax.random.fold_in(own, 2), (rows, 1), 0, top)
    return jnp.take_along_axis(table, (jnp.arange(top)[None, :] + offset_by) % top, axis=1)


def portions_of(count, total, limit, skew, full):
    loads = [(1 << 20) // math.isqrt(rank ** skew) + 1 for rank in range(1, count + 1)]
    largest = limit if full else min(limit, max(-(-total // count), total * loads[0] // sum(loads)))
    least = 1 if total - largest >= count - 1 else 0
    holding, spare = [largest] + [least] * (count - 1), total - largest - least * (count - 1)
    while spare > 0:
        free = [i for i in range(1, count) if holding[i] < largest] or [i for i in range(1, count) if holding[i] < limit]
        pool, left = sum([loads[i] for i in free]), spare
        for i in free:
            extra = min(limit - holding[i], max(1, left * loads[i] // pool), spare)
            holding[i] = holding[i] + extra
            spare = spare - extra
    return np.array(holding)


def normal_values(rng, dims, width, reach, cuts=(), held_as=jnp.bfloat16):
    gain = shard_levels(rng, dims, cuts, -0.22, 0.18) if cuts else 1.0
    array = jax.random.normal(rng, dims, jnp.float32) * width * gain
    return jnp.minimum(jnp.maximum(array, -reach), reach).astype(held_as)


def setup_inputs(seed: int = 0) -> dict:
    seeds = jax.random.split(jax.random.key(seed), 7)
    tokens = normal_values(seeds[0], (TOKENS, D), 1.0, 6.0, ((0, 32), (1, 8)))
    expert_ids_keys = jax.random.split(jax.random.fold_in(seeds[1], 1), TOKENS // TOK_DEV)
    expert_ids_turns = jax.random.permutation(jax.random.fold_in(seeds[1], 3), TOKENS // TOK_DEV)
    expert_ids = jax.vmap(lambda own, number: assign_block(jax.random.fold_in(seeds[1], 2), own, number, TOK_DEV, EXPERTS, TOP, CAP, 2))(expert_ids_keys, expert_ids_turns).reshape((TOKENS, TOP))
    combine_weights = jnp.clip(jnp.exp(math.log(0.6) - 2.4849067 * jax.random.uniform(seeds[2], (TOKENS, TOP), jnp.float32) ** shard_levels(seeds[2], (TOKENS, TOP), ((0, 32),), -0.2, 0.2)), 0.05, 0.6)
    gate_weight = normal_values(seeds[3], (EXPERTS, D, FF), D ** -0.5, 0.109375, ((0, 32), (2, 8)))
    up_weight = normal_values(seeds[4], (EXPERTS, D, FF), D ** -0.5, 0.109375, ((0, 32), (2, 8)))
    down_weight = normal_values(seeds[5], (EXPERTS, FF, D), FF ** -0.5, 0.109375, ((0, 32), (1, 8)))
    return {"tokens": tokens, "expert_ids": expert_ids, "combine_weights": combine_weights, "gate_weight": gate_weight, "up_weight": up_weight, "down_weight": down_weight}


def activate(gate_acc, up_acc):
    return (up_acc + 1.0) * gate_acc * jax.nn.sigmoid(1.702 * gate_acc)


def reference(tokens, expert_ids, combine_weights, gate_weight, up_weight, down_weight):
    groups = expert_ids.reshape(N_EP, TOK_DEV * TOP)
    onehot = (groups[:, :, None] == jnp.arange(EXPERTS, dtype=jnp.int32)[None, None, :]).astype(jnp.int32)
    slot_pos = jnp.sum((jnp.cumsum(onehot, axis=1) - onehot) * onehot, axis=2)
    group_ids = jnp.arange(N_EP, dtype=jnp.int32)[:, None]
    flat_slot = ((groups * N_EP + group_ids) * CAP + slot_pos).reshape(-1)
    token_idx = (group_ids * TOK_DEV + jnp.arange(TOK_DEV * TOP, dtype=jnp.int32)[None, :] // TOP).reshape(-1)
    token_src = jnp.zeros((EXPERTS * N_EP * CAP,), jnp.int32).at[flat_slot].set(token_idx)
    slot_weight = jnp.zeros((EXPERTS * N_EP * CAP,), jnp.float32).at[flat_slot].set(combine_weights.reshape(-1))
    token_src = token_src.reshape(EXPERTS, N_EP * CAP)
    slot_weight = slot_weight.reshape(EXPERTS, N_EP * CAP)

    def per_expert(accum, inputs):
        row_src, row_weight, gate_cols, up_cols, down_rows = inputs
        row_data = tokens[row_src]
        gate_acc = jnp.dot(row_data, gate_cols, preferred_element_type=jnp.float32)
        up_acc = jnp.dot(row_data, up_cols, preferred_element_type=jnp.float32)
        hidden = activate(gate_acc, up_acc).astype(jnp.bfloat16)
        partials = jnp.einsum("rtf,tfd->rtd",
                              hidden.reshape(N_EP * CAP, N_TP, FF_DEV).astype(jnp.float32),
                              down_rows.reshape(N_TP, FF_DEV, D).astype(jnp.float32))
        rounded = lax.optimization_barrier(partials.astype(jnp.bfloat16))
        expert_out = jnp.sum(rounded.astype(jnp.float32), axis=1)
        accum = accum.at[row_src].add(row_weight[:, None] * expert_out)
        return accum, None

    accum = jnp.zeros((TOKENS, D), jnp.float32)
    accum, unused = lax.scan(per_expert, accum, (token_src, slot_weight, gate_weight, up_weight, down_weight))
    return accum.astype(jnp.bfloat16)
```

```python
import jax
import jax.numpy as jnp
from jax import lax
from jax.experimental import pallas as pl
from jax.experimental.pallas import tpu as pltpu
from jax.sharding import Mesh
from jax.sharding import PartitionSpec as P


PARTS = (16, 16)
CORES = 2
RING = 4
LANES = 384
HALF = 368
BLOCK = 256
VMEM = 56 * 1024 * 1024

f32, bf16 = jnp.float32, jnp.bfloat16
NT = (((1,), (1,)), ((), ()))
TN = (((0,), (0,)), ((), ()))


def slots_of(ids, experts):
    top, toks = ids.shape
    j = lax.broadcasted_iota(jnp.int32, (experts, toks), 0)
    chips = experts // CORES
    expert = CORES * lax.rem(j, chips) + lax.div(j, chips)
    hit = [ids[k : k + 1, :] == expert for k in range(top)]
    member = sum(h.astype(f32) for h in hit)
    before = lax.broadcasted_iota(jnp.int32, (toks, toks), 0) < lax.broadcasted_iota(jnp.int32, (toks, toks), 1)
    rank = jnp.dot(member.astype(bf16), before.astype(f32).astype(bf16), preferred_element_type=f32)
    return hit, jnp.where(member > 0, rank, -1.0)


def spread(rank, start, size):
    experts, toks = rank.shape
    slot = lax.broadcasted_iota(jnp.int32, (experts, size, toks), 1).astype(f32) + float(start)
    wide = jnp.broadcast_to(rank[:, None, :], (experts, size, toks))
    return wide == slot


def dispatch(ids_t, tok_t, experts, start, size):
    feats, toks = tok_t.shape

    def body(ids_ref, tok_ref, out_ref, pad_ref):
        pad_ref[...] = jnp.zeros(pad_ref.shape, bf16)
        pad_ref[:feats, :] = tok_ref[...]
        _, rank = slots_of(ids_ref[...], experts)
        pick = spread(rank, start, size).astype(f32).reshape(experts * size, toks).astype(bf16)
        out_ref[...] = lax.dot_general(pick, pad_ref[...], NT, preferred_element_type=f32).astype(bf16)

    return pl.pallas_call(
        body,
        out_shape=jax.ShapeDtypeStruct((experts * size, LANES), bf16),
        scratch_shapes=[pltpu.VMEM((LANES, toks), bf16)],
        compiler_params=pltpu.CompilerParams(vmem_limit_bytes=VMEM),
        name=f"dispatch_{start}",
    )(ids_t, tok_t)


def combine(ids_t, cw_t, rows, acc, experts, start, size, feats):
    toks = ids_t.shape[1]
    last = feats is not None

    def body(*refs):
        ids_ref, cw_ref, rows_ref = refs[:3]
        out_ref = refs[-1]
        hit, rank = slots_of(ids_ref[...], experts)
        cw = cw_ref[...]
        weight = sum(jnp.where(h, cw[k : k + 1, :], 0.0) for k, h in enumerate(hit))
        wide = jnp.broadcast_to(weight[:, None, :], (experts, size, toks))
        coef = jnp.where(spread(rank, start, size), wide, 0.0).reshape(experts * size, toks)
        high = coef.astype(bf16)
        low = (coef - high.astype(f32)).astype(bf16)
        total = lax.dot_general(high, rows_ref[...], TN, preferred_element_type=f32)
        total += lax.dot_general(low, rows_ref[...], TN, preferred_element_type=f32)
        if acc is not None:
            total += refs[3][...]
        if last:
            out_ref[...] = total.T[:feats, :].astype(bf16)
        else:
            out_ref[...] = total

    out = jax.ShapeDtypeStruct((feats, toks), bf16) if last else jax.ShapeDtypeStruct((toks, LANES), f32)
    return pl.pallas_call(
        body,
        out_shape=out,
        compiler_params=pltpu.CompilerParams(vmem_limit_bytes=VMEM),
        name=f"combine_{start}",
    )(ids_t, cw_t, rows, *(() if acc is None else (acc,)))


def arrange(core, own, received):
    _, units, width = own.shape
    count = RING * CORES
    feats = width // count

    def body(core_ref, own_ref, recv_ref, out_ref):
        out_ref[...] = jnp.zeros(out_ref.shape, bf16)
        for j in range(count):
            out_ref[j, :units, :feats] = own_ref[0, :, j * feats : (j + 1) * feats]
            out_ref[j, HALF : HALF + units, :feats] = recv_ref[:, j * feats : (j + 1) * feats]

    return pl.pallas_call(
        body,
        grid_spec=pltpu.PrefetchScalarGridSpec(
            num_scalar_prefetch=1,
            grid=(1,),
            in_specs=[
                pl.BlockSpec((1, units, width), lambda i, c: (c[0], 0, 0)),
                pl.BlockSpec((units, width), lambda i, c: (0, 0)),
            ],
            out_specs=pl.BlockSpec((count, 2 * HALF, LANES), lambda i, c: (0, 0, 0)),
        ),
        out_shape=jax.ShapeDtypeStruct((count, 2 * HALF, LANES), bf16),
        compiler_params=pltpu.CompilerParams(vmem_limit_bytes=VMEM),
        name="arrange",
    )(core, own, received)


def expert(row, pieces, gate_w, up_w, down_w):
    keys = sorted(pieces)
    rows = pieces[keys[0]].shape[0]
    count = len(keys)

    def body(row_ref, *refs):
        xs, (g_ref, u_ref, d_ref), outs = refs[:count], refs[count : count + 3], refs[count + 3 :]
        at = [CORES * lax.rem(row_ref[0] + k, RING) + c for k, c in keys]
        gate = up = 0.0
        for x_ref, j in zip(xs, at):
            x = x_ref[...]
            gate += lax.dot_general(x, g_ref[j], NT, preferred_element_type=f32)
            up += lax.dot_general(x, u_ref[j], NT, preferred_element_type=f32)
        hidden = ((up + 1.0) * gate * jax.nn.sigmoid(1.702 * gate)).astype(bf16)
        for out_ref, j in zip(outs, at):
            out_ref[...] = jnp.dot(hidden, d_ref[j], preferred_element_type=f32).astype(bf16)

    rows_spec = pl.BlockSpec((BLOCK, LANES), lambda i, r: (i, 0))
    weight_spec = pl.BlockSpec((count, 2 * HALF, LANES), lambda i, r: (0, 0, 0))
    outs = pl.pallas_call(
        body,
        grid_spec=pltpu.PrefetchScalarGridSpec(
            num_scalar_prefetch=1,
            grid=(rows // BLOCK,),
            in_specs=[rows_spec] * count + [weight_spec] * 3,
            out_specs=[rows_spec] * count,
        ),
        out_shape=[jax.ShapeDtypeStruct((rows, LANES), bf16)] * count,
        compiler_params=pltpu.CompilerParams(vmem_limit_bytes=VMEM),
        name="expert",
    )(row, *(pieces[k] for k in keys), gate_w, up_w, down_w)
    return dict(zip(keys, outs))


def shift(array, by):
    return lax.ppermute(array, "y", [(i, (i + by) % RING) for i in range(RING)])


def gathered(own):
    half = own.shape[0] // CORES
    a, b = own[:half], own[half:]
    back_a, fore_b = shift(a, 1), shift(b, -1)
    back_b, fore_a = shift(b, 1), shift(a, -1)
    far_a, far_b = shift(back_a, 1), shift(fore_b, -1)
    return {
        (0, 0): a, (0, 1): b,
        (1, 0): fore_a, (1, 1): fore_b,
        (2, 0): far_a, (2, 1): far_b,
        (3, 0): back_a, (3, 1): back_b,
    }


def added(*parts):
    return sum(p.astype(f32) for p in parts).astype(bf16)


def scattered(part):
    via_a, via_b = shift(part[2, 0], 1), shift(part[2, 1], -1)
    back_b, fore_a = shift(part[1, 1], 1), shift(part[3, 0], -1)
    back_a = shift(added(part[1, 0], via_a), 1)
    fore_b = shift(added(part[3, 1], via_b), -1)
    return jnp.concatenate([added(part[0, 0], back_a, fore_a), added(part[0, 1], back_b, fore_b)])


def exchange(array):
    return lax.all_to_all(array, ("c", "x", "z"), 0, 0, tiled=True)


def local(tokens, expert_ids, combine_weights, gate_weight, up_weight, down_weight):
    experts = gate_weight.shape[0] * lax.axis_size(("x", "z"))
    feats = tokens.shape[1]
    core = lax.axis_index("c").astype(jnp.int32)
    row = lax.axis_index("y").astype(jnp.int32)[None]
    tok_t, ids_t, cw_t = tokens.T, expert_ids.T, combine_weights.T

    arranged = []
    for w in (gate_weight.swapaxes(1, 2), up_weight.swapaxes(1, 2), down_weight):
        other = lax.dynamic_index_in_dim(w, 1 - core, 0, keepdims=False)
        arranged.append(arrange(core[None], w, lax.ppermute(other, "c", [(0, 1), (1, 0)])))

    starts = [sum(PARTS[:i]) for i in range(len(PARTS))]
    returned = []
    for start, size in zip(starts, PARTS):
        sent = dispatch(ids_t, tok_t, experts, start, size)
        part = expert(row, gathered(exchange(sent)), *arranged)
        returned.append(exchange(scattered(part)))
    acc = None
    for i, (start, size) in enumerate(zip(starts, PARTS)):
        last = i == len(PARTS) - 1
        acc = combine(ids_t, cw_t, returned[i], acc, experts, start, size, feats if last else None)
    return acc.T


def solution(mesh):
    split = Mesh(mesh.devices.reshape(4, -1, RING, CORES), ("x", "z", "y", "c"))
    ep, tp = ("x", "z"), ("y", "c")
    placed = (P(ep, tp), P(ep, None), P(ep, None), P(ep, None, tp), P(ep, None, tp), P(ep, tp, None))
    return jax.shard_map(local, mesh=split, in_specs=placed, out_specs=P(ep, tp), check_vma=False)
```

```python
import jax
import jax.numpy as jnp
from jax import lax
from jax.experimental import pallas as pl
from jax.experimental.pallas import tpu as pltpu
from jax.sharding import Mesh
from jax.sharding import PartitionSpec as P


PARTS = (16, 16)
CORES = 2
RING = 4
LANES = 384
HALF = 368
GROUP = 32
WIDE = CORES * LANES
VMEM = 56 * 1024 * 1024

f32, bf16 = jnp.float32, jnp.bfloat16
NT = (((1,), (1,)), ((), ()))


def lasting(us):
    return pl.CostEstimate(flops=int(us * 250_000_000), bytes_accessed=0, transcendentals=0)


def slots_of(ids, experts):
    top, toks = ids.shape
    j = lax.broadcasted_iota(jnp.int32, (experts, toks), 0)
    chips = experts // CORES
    named = CORES * lax.rem(j, chips) + lax.div(j, chips)
    hit = [ids[k : k + 1, :] == named for k in range(top)]
    member = sum(h.astype(f32) for h in hit)
    before = lax.broadcasted_iota(jnp.int32, (toks, toks), 0) < lax.broadcasted_iota(jnp.int32, (toks, toks), 1)
    rank = jnp.dot(member.astype(bf16), before.astype(f32).astype(bf16), preferred_element_type=f32)
    return hit, jnp.where(member > 0, rank, -1.0)


def spread(rank, start, size):
    some, toks = rank.shape
    slot = lax.broadcasted_iota(jnp.int32, (some, size, toks), 1).astype(f32) + float(start)
    return jnp.broadcast_to(rank[:, None, :], (some, size, toks)) == slot


def dispatch(ids_t, tok_t, experts, start, size):
    feats, toks = tok_t.shape

    def body(ids_ref, tok_ref, out_ref, pad_ref, rank_ref):
        pad_ref[...] = jnp.zeros(pad_ref.shape, bf16)
        pad_ref[:feats, :] = tok_ref[...]
        rank_ref[...] = slots_of(ids_ref[...], experts)[1]

        @pl.loop(0, experts // GROUP)
        def _(i):
            rank = rank_ref[pl.ds(pl.multiple_of(i * GROUP, GROUP), GROUP), :]
            pick = spread(rank, start, size).astype(f32).reshape(GROUP * size, toks).astype(bf16)
            rows = lax.dot_general(pick, pad_ref[...], NT, preferred_element_type=f32)
            out_ref[pl.ds(pl.multiple_of(i * GROUP * size, GROUP * size), GROUP * size), :] = rows.astype(bf16)

    return pl.pallas_call(
        body,
        out_shape=jax.ShapeDtypeStruct((experts * size, LANES), bf16),
        scratch_shapes=[pltpu.VMEM((LANES, toks), bf16), pltpu.VMEM((experts, toks), f32)],
        compiler_params=pltpu.CompilerParams(vmem_limit_bytes=VMEM),
        cost_estimate=lasting(3),
    )(ids_t, tok_t)


def factors(ids_t, cw_t, experts, start, size):
    toks = ids_t.shape[1]

    def body(ids_ref, cw_ref, high_ref, low_ref, rank_ref, weight_ref):
        hit, rank_ref[...] = slots_of(ids_ref[...], experts)
        cw = cw_ref[...]
        weight_ref[...] = sum(jnp.where(h, cw[k : k + 1, :], 0.0) for k, h in enumerate(hit))

        @pl.loop(0, experts // GROUP)
        def _(i):
            some = pl.ds(pl.multiple_of(i * GROUP, GROUP), GROUP)
            wide = jnp.broadcast_to(weight_ref[some, :][:, None, :], (GROUP, size, toks))
            coef = jnp.where(spread(rank_ref[some, :], start, size), wide, 0.0).reshape(GROUP * size, toks).T
            high = coef.astype(bf16)
            at = pl.ds(pl.multiple_of(i * GROUP * size, GROUP * size), GROUP * size)
            high_ref[:, at] = high
            low_ref[:, at] = (coef - high.astype(f32)).astype(bf16)

    return pl.pallas_call(
        body,
        out_shape=[jax.ShapeDtypeStruct((toks, experts * size), bf16)] * 2,
        scratch_shapes=[pltpu.VMEM((experts, toks), f32)] * 2,
        compiler_params=pltpu.CompilerParams(vmem_limit_bytes=VMEM),
        cost_estimate=lasting(4),
    )(ids_t, cw_t)


def combine(rows, parts, acc, feats):
    toks = parts[0].shape[0]
    last = feats is not None

    def body(rows_ref, high_ref, low_ref, *refs):
        out_ref = refs[-1]
        total = jnp.dot(high_ref[...], rows_ref[...], preferred_element_type=f32)
        total += jnp.dot(low_ref[...], rows_ref[...], preferred_element_type=f32)
        if acc is not None:
            total += refs[0][...]
        out_ref[...] = total.T[:feats, :].astype(bf16) if last else total

    return pl.pallas_call(
        body,
        out_shape=jax.ShapeDtypeStruct((feats, toks), bf16) if last else jax.ShapeDtypeStruct((toks, LANES), f32),
        compiler_params=pltpu.CompilerParams(vmem_limit_bytes=VMEM),
        cost_estimate=lasting(2),
        name="combine",
    )(rows, *parts, *(() if acc is None else (acc,)))


def arrange(core, own, received):
    _, units, width = own.shape
    feats = width // (RING * CORES)

    def body(core_ref, own_ref, recv_ref, out_ref):
        for first in (0, HALF):
            out_ref[0, first + units : first + HALF, :] = jnp.zeros((HALF - units, WIDE), bf16)
        for c in range(CORES):
            out_ref[0, :, c * LANES + feats : (c + 1) * LANES] = jnp.zeros((2 * HALF, LANES - feats), bf16)
        for q in range(RING):

            @pl.when(pl.program_id(0) == q)
            def _(q=q):
                for c in range(CORES):
                    j = (CORES * q + c) * feats
                    to = slice(c * LANES, c * LANES + feats)
                    out_ref[0, :units, to] = own_ref[0, :, j : j + feats]
                    out_ref[0, HALF : HALF + units, to] = recv_ref[:, j : j + feats]

    return pl.pallas_call(
        body,
        grid_spec=pltpu.PrefetchScalarGridSpec(
            num_scalar_prefetch=1,
            grid=(RING,),
            in_specs=[
                pl.BlockSpec((1, units, width), lambda i, c: (c[0], 0, 0)),
                pl.BlockSpec((units, width), lambda i, c: (0, 0)),
            ],
            out_specs=pl.BlockSpec((1, 2 * HALF, WIDE), lambda i, c: (i, 0, 0)),
        ),
        out_shape=jax.ShapeDtypeStruct((RING, 2 * HALF, WIDE), bf16),
        compiler_params=pltpu.CompilerParams(vmem_limit_bytes=VMEM),
        cost_estimate=lasting(6),
        name="arrange",
    )(core, own, received)


CAME = [((0, 0), (0, 1)), ((1, 0), (1, 1)), ((3, 0), (3, 1)), ((2, 0),), ((2, 1),)]
GOES = [((0, 0), (0, 1)), ((2, 0), (1, 1)), ((2, 1), (3, 0)), ((1, 0),), ((3, 1),)]


def copies(row, arrays, keys, buf, sem, out, only=None):
    for i, (ref, blocks) in enumerate(zip(arrays, keys)):
        for b, (k, c) in enumerate(blocks):
            if only is None or only == k:
                here = buf.at[lax.rem(row + k, RING), :, pl.ds(c * LANES, LANES)]
                ends = (here, ref.at[b]) if out else (ref.at[b], here)
                yield pltpu.make_async_copy(*ends, sem.at[i, b])


def kernel(body, inputs, out_shape, scratch, us):
    hbm = pl.BlockSpec(memory_space=pltpu.MemorySpace.HBM)
    many = isinstance(out_shape, list)
    return pl.pallas_call(
        body,
        in_specs=[pl.BlockSpec(memory_space=pltpu.MemorySpace.SMEM)] + [hbm] * (len(inputs) - 1),
        out_specs=[hbm] * len(out_shape) if many else pl.BlockSpec(memory_space=pltpu.MemorySpace.VMEM),
        out_shape=out_shape,
        scratch_shapes=scratch,
        compiler_params=pltpu.CompilerParams(vmem_limit_bytes=VMEM),
        cost_estimate=lasting(us),
    )(*inputs)


def lift(row, pieces, gate_w, up_w):
    h = pieces[0].shape[1]
    units = gate_w.shape[1]

    def body(row_ref, *refs):
        xs, ws, out_ref = refs[:5], refs[5:7], refs[7]
        x, g, u, gate, up, xsem, wsem = refs[8:]
        row = row_ref[0]

        def load(w, k):
            j = lax.rem(row + k, RING)
            return pltpu.make_async_copy(ws[w].at[j], (g, u)[w].at[j], wsem.at[w, k])

        for k in range(RING):
            for cp in copies(row, xs, CAME, x, xsem, False, k):
                cp.start()
            load(0, k).start()
            load(1, k).start()
        gate[...] = jnp.zeros(gate.shape, f32)
        up[...] = jnp.zeros(up.shape, f32)

        @pl.loop(0, RING)
        def _(k):
            j = lax.rem(row + k, RING)
            for some in range(RING):

                @pl.when(k == some)
                def _(some=some):
                    for cp in copies(row, xs, CAME, x, xsem, False, some):
                        cp.wait()

            load(0, k).wait()
            gate[...] += lax.dot_general(x[j], g[j], NT, preferred_element_type=f32)
            load(1, k).wait()
            up[...] += lax.dot_general(x[j], u[j], NT, preferred_element_type=f32)

        a = gate[...]
        out_ref[...] = ((up[...] + 1.0) * a * jax.nn.sigmoid(1.702 * a)).astype(bf16)

    return kernel(
        body,
        (row, *pieces, gate_w, up_w),
        jax.ShapeDtypeStruct((h, units), bf16),
        [pltpu.VMEM((RING, h, WIDE), bf16)]
        + [pltpu.VMEM(gate_w.shape, bf16)] * 2
        + [pltpu.VMEM((h, units), f32)] * 2
        + [pltpu.SemaphoreType.DMA((5, 2)), pltpu.SemaphoreType.DMA((2, RING))],
        9 * h // 512,
    )


def lower(row, hidden, down_w):
    h = hidden.shape[0]

    def body(row_ref, hid_ref, w_ref, *refs):
        outs = refs[:5]
        hid, d, y, hsem, wsem, ysem = refs[5:]
        row = row_ref[0]
        fetch = pltpu.make_async_copy(hid_ref, hid, hsem)
        fetch.start()

        def load(k):
            j = lax.rem(row + k, RING)
            return pltpu.make_async_copy(w_ref.at[j], d.at[j], wsem.at[k])

        for k in range(RING):
            load(RING - 1 - k).start()
        fetch.wait()

        @pl.loop(0, RING)
        def _(i):
            k = RING - 1 - i
            j = lax.rem(row + k, RING)
            load(k).wait()
            y[j] = jnp.dot(hid[...], d[j], preferred_element_type=f32).astype(bf16)
            for some in range(RING):

                @pl.when(k == some)
                def _(some=some):
                    for cp in copies(row, outs, GOES, y, ysem, True, some):
                        cp.start()

        for cp in copies(row, outs, GOES, y, ysem, True):
            cp.wait()

    return kernel(
        body,
        (row, hidden, down_w),
        [jax.ShapeDtypeStruct((len(k), h, LANES), bf16) for k in GOES],
        [pltpu.VMEM(hidden.shape, bf16), pltpu.VMEM(down_w.shape, bf16), pltpu.VMEM((RING, h, WIDE), bf16)]
        + [pltpu.SemaphoreType.DMA, pltpu.SemaphoreType.DMA((RING,)), pltpu.SemaphoreType.DMA((5, 2))],
        5 * h // 512,
    )


def shift(array, by):
    return lax.ppermute(array, "y", [(i, (i + by) % RING) for i in range(RING)])


def gathered(own):
    own = own.reshape(CORES, -1, LANES)
    back, fore = shift(own, 1), shift(own, -1)
    far_a, far_b = shift(back[:1], 1), shift(fore[1:], -1)
    return own, fore, back, far_a, far_b


def added(*parts):
    return sum(p.astype(f32) for p in parts).astype(bf16)


def scattered(parts):
    own, plus, minus, later_a, later_b = parts
    plus, minus = shift(plus, 1), shift(minus, -1)
    back_a = shift(added(later_a, plus[:1]), 1)
    fore_b = shift(added(later_b, minus[:1]), -1)
    total = jnp.concatenate([added(own[:1], minus[1:], back_a), added(own[1:], plus[1:], fore_b)])
    return total.reshape(-1, LANES)


def exchange(array):
    return lax.all_to_all(array, ("c", "x", "z"), 0, 0, tiled=True)


def local(tokens, expert_ids, combine_weights, gate_weight, up_weight, down_weight):
    experts = gate_weight.shape[0] * lax.axis_size(("x", "z"))
    feats = tokens.shape[1]
    core = lax.axis_index("c").astype(jnp.int32)
    row = lax.axis_index("y").astype(jnp.int32)[None]
    tok_t, ids_t, cw_t = tokens.T, expert_ids.T, combine_weights.T

    arranged = []
    for w in (gate_weight.swapaxes(1, 2), up_weight.swapaxes(1, 2), down_weight):
        other = lax.dynamic_index_in_dim(w, 1 - core, 0, keepdims=False)
        other = lax.ppermute(other, "c", [(0, 1), (1, 0)])
        arranged.append(arrange(core[None], w, other))

    returned, parts = [], []
    for i, size in enumerate(PARTS):
        start = sum(PARTS[:i])
        sent = dispatch(ids_t, tok_t, experts, start, size)
        sent = exchange(sent)
        pieces = gathered(sent)
        hidden = lift(row, pieces, *arranged[:2])
        part = lower(row, hidden, arranged[2])
        part = scattered(part)
        returned.append(exchange(part))
        parts.append(factors(ids_t, cw_t, experts, start, size))
    acc = None
    for i in range(len(PARTS)):
        acc = combine(returned[i], parts[i], acc, feats if i == len(PARTS) - 1 else None)
    return acc.T


def solution(mesh):
    split = Mesh(mesh.devices.reshape(4, -1, RING, CORES), ("x", "z", "y", "c"))
    ep, tp = ("x", "z"), ("y", "c")
    placed = (P(ep, tp), P(ep, None), P(ep, None), P(ep, None, tp), P(ep, None, tp), P(ep, tp, None))

    return jax.shard_map(local, mesh=split, in_specs=placed, out_specs=P(ep, tp), check_vma=False)
```

```python
import jax
import jax.numpy as jnp
from jax import lax
from jax.experimental import pallas as pl
from jax.experimental.pallas import tpu as pltpu
from jax.sharding import Mesh
from jax.sharding import PartitionSpec as P


PARTS = (16, 16)
CORES = 2
RING = 4
LANES = 384
HALF = 368
STEP = 112
GROUP = 32
WIDE = CORES * LANES
VMEM = 56 * 1024 * 1024

f32, bf16 = jnp.float32, jnp.bfloat16
NT = (((1,), (1,)), ((), ()))


def lasting(us):
    return pl.CostEstimate(flops=int(us * 250_000_000), bytes_accessed=0, transcendentals=0)


def slots_of(ids, experts):
    top, toks = ids.shape
    j = lax.broadcasted_iota(jnp.int32, (experts, toks), 0)
    chips = experts // CORES
    named = CORES * lax.rem(j, chips) + lax.div(j, chips)
    hit = [ids[k : k + 1, :] == named for k in range(top)]
    member = sum(h.astype(f32) for h in hit)
    before = lax.broadcasted_iota(jnp.int32, (toks, toks), 0) < lax.broadcasted_iota(jnp.int32, (toks, toks), 1)
    rank = jnp.dot(member.astype(bf16), before.astype(f32).astype(bf16), preferred_element_type=f32)
    return hit, jnp.where(member > 0, rank, -1.0)


def spread(rank, start, size):
    some, toks = rank.shape
    slot = lax.broadcasted_iota(jnp.int32, (some, size, toks), 1).astype(f32) + float(start)
    return jnp.broadcast_to(rank[:, None, :], (some, size, toks)) == slot


def dispatch(ids_t, tok_t, experts, start, size):
    feats, toks = tok_t.shape

    def body(ids_ref, tok_ref, out_ref, pad_ref, rank_ref):
        pad_ref[...] = jnp.zeros(pad_ref.shape, bf16)
        pad_ref[:feats, :] = tok_ref[...]
        rank_ref[...] = slots_of(ids_ref[...], experts)[1]

        @pl.loop(0, experts // GROUP)
        def _(i):
            rank = rank_ref[pl.ds(pl.multiple_of(i * GROUP, GROUP), GROUP), :]
            pick = spread(rank, start, size).astype(f32).reshape(GROUP * size, toks).astype(bf16)
            rows = lax.dot_general(pick, pad_ref[...], NT, preferred_element_type=f32)
            out_ref[pl.ds(pl.multiple_of(i * GROUP * size, GROUP * size), GROUP * size), :] = rows.astype(bf16)

    return pl.pallas_call(
        body,
        out_shape=jax.ShapeDtypeStruct((experts * size, LANES), bf16),
        scratch_shapes=[pltpu.VMEM((LANES, toks), bf16), pltpu.VMEM((experts, toks), f32)],
        compiler_params=pltpu.CompilerParams(vmem_limit_bytes=VMEM),
        cost_estimate=lasting(3),
    )(ids_t, tok_t)


def factors(ids_t, cw_t, experts, start, size):
    toks = ids_t.shape[1]

    def body(ids_ref, cw_ref, out_ref, rank_ref, weight_ref):
        hit, rank_ref[...] = slots_of(ids_ref[...], experts)
        cw = cw_ref[...]
        weight_ref[...] = sum(jnp.where(h, cw[k : k + 1, :], 0.0) for k, h in enumerate(hit))

        @pl.loop(0, experts // GROUP)
        def _(i):
            some = pl.ds(pl.multiple_of(i * GROUP, GROUP), GROUP)
            wide = jnp.broadcast_to(weight_ref[some, :][:, None, :], (GROUP, size, toks))
            coef = jnp.where(spread(rank_ref[some, :], start, size), wide, 0.0).reshape(GROUP * size, toks).T
            high = coef.astype(bf16)
            at = pl.ds(pl.multiple_of(i * GROUP * size, GROUP * size), GROUP * size)
            out_ref[0, :, at] = high
            out_ref[1, :, at] = (coef - high.astype(f32)).astype(bf16)

    return pl.pallas_call(
        body,
        out_shape=jax.ShapeDtypeStruct((2, toks, experts * size), bf16),
        scratch_shapes=[pltpu.VMEM((experts, toks), f32)] * 2,
        compiler_params=pltpu.CompilerParams(vmem_limit_bytes=VMEM),
        cost_estimate=lasting(4),
    )(ids_t, cw_t)


def combine(rows, parts, acc, feats):
    toks = parts.shape[1]
    last = feats is not None

    def body(rows_ref, parts_ref, *refs):
        out_ref, sum_ref = refs[-2:]
        sum_ref[...] = jnp.zeros(sum_ref.shape, f32) if acc is None else refs[0][...]

        @pl.loop(0, 2)
        def _(p):
            sum_ref[...] += jnp.dot(parts_ref[p], rows_ref[...], preferred_element_type=f32)

        out_ref[...] = sum_ref[...].T[:feats, :].astype(bf16) if last else sum_ref[...]

    return pl.pallas_call(
        body,
        out_shape=jax.ShapeDtypeStruct((feats, toks), bf16) if last else jax.ShapeDtypeStruct((toks, LANES), f32),
        scratch_shapes=[pltpu.VMEM((toks, LANES), f32)],
        compiler_params=pltpu.CompilerParams(vmem_limit_bytes=VMEM),
        cost_estimate=lasting(2),
        name="combine",
    )(rows, parts, *(() if acc is None else (acc,)))


def arrange(core, own, received):
    _, units, width = own.shape
    feats = width // (RING * CORES)

    def body(core_ref, own_ref, recv_ref, out_ref):
        for first in (0, HALF):
            out_ref[0, first + units : first + HALF, :] = jnp.zeros((HALF - units, WIDE), bf16)
        for c in range(CORES):
            out_ref[0, :, c * LANES + feats : (c + 1) * LANES] = jnp.zeros((2 * HALF, LANES - feats), bf16)
        for q in range(RING):

            @pl.when(pl.program_id(0) == q)
            def _(q=q):
                def move(at, size):
                    for c in range(CORES):
                        j = (CORES * q + c) * feats
                        to = slice(c * LANES, c * LANES + feats)
                        out_ref[0, pl.ds(at, size), to] = own_ref[0, pl.ds(at, size), j : j + feats]
                        out_ref[0, pl.ds(HALF + at, size), to] = recv_ref[pl.ds(at, size), j : j + feats]

                @pl.loop(0, units // STEP)
                def _(i):
                    move(pl.multiple_of(i * STEP, STEP), STEP)

                if units % STEP:
                    move(units - units % STEP, units % STEP)

    return pl.pallas_call(
        body,
        grid_spec=pltpu.PrefetchScalarGridSpec(
            num_scalar_prefetch=1,
            grid=(RING,),
            in_specs=[
                pl.BlockSpec((1, units, width), lambda i, c: (c[0], 0, 0)),
                pl.BlockSpec((units, width), lambda i, c: (0, 0)),
            ],
            out_specs=pl.BlockSpec((1, 2 * HALF, WIDE), lambda i, c: (i, 0, 0)),
        ),
        out_shape=jax.ShapeDtypeStruct((RING, 2 * HALF, WIDE), bf16),
        compiler_params=pltpu.CompilerParams(vmem_limit_bytes=VMEM),
        cost_estimate=lasting(6),
        name="arrange",
    )(core, own, received)


CAME = [((0, 0), (0, 1)), ((3, 0),), ((1, 1),), ((3, 1),), ((1, 0),), ((2, 0),), ((2, 1),)]
GOES = [((0, 0), (0, 1)), ((2, 0),), ((2, 1),), ((1, 1),), ((3, 0),), ((1, 0),), ((3, 1),)]
MANY = len(CAME)


def copies(row, arrays, keys, buf, sem, out, only=None):
    for i, (ref, blocks) in enumerate(zip(arrays, keys)):
        for b, (k, c) in enumerate(blocks):
            if only is None or only == k:
                here = buf.at[lax.rem(row + k, RING), :, pl.ds(c * LANES, LANES)]
                ends = (here, ref.at[b]) if out else (ref.at[b], here)
                yield pltpu.make_async_copy(*ends, sem.at[i, b])


def kernel(body, inputs, out_shape, scratch, us):
    hbm = pl.BlockSpec(memory_space=pltpu.MemorySpace.HBM)
    many = isinstance(out_shape, list)
    return pl.pallas_call(
        body,
        in_specs=[pl.BlockSpec(memory_space=pltpu.MemorySpace.SMEM)] + [hbm] * (len(inputs) - 1),
        out_specs=[hbm] * len(out_shape) if many else pl.BlockSpec(memory_space=pltpu.MemorySpace.VMEM),
        out_shape=out_shape,
        scratch_shapes=scratch,
        compiler_params=pltpu.CompilerParams(vmem_limit_bytes=VMEM),
        cost_estimate=lasting(us),
    )(*inputs)


def lift(row, pieces, gate_w, up_w):
    h = pieces[0].shape[1]
    units = gate_w.shape[1]

    def body(row_ref, *refs):
        xs, ws, out_ref = refs[:MANY], refs[MANY : MANY + 2], refs[MANY + 2]
        x, gu, acc, xsem, wsem = refs[MANY + 3 :]
        row = row_ref[0]

        def load(w, k):
            j = lax.rem(row + k, RING)
            return pltpu.make_async_copy(ws[w].at[j], gu.at[w, j], wsem.at[w, k])

        for k in range(RING):
            for cp in copies(row, xs, CAME, x, xsem, False, k):
                cp.start()
            load(0, k).start()
            load(1, k).start()
        acc[...] = jnp.zeros(acc.shape, f32)

        @pl.loop(0, 2 * RING)
        def _(i):
            k, w = lax.div(i, 2), lax.rem(i, 2)
            j = lax.rem(row + k, RING)
            for some in range(RING):

                @pl.when(i == 2 * some)
                def _(some=some):
                    for cp in copies(row, xs, CAME, x, xsem, False, some):
                        cp.wait()

            for some in range(2):

                @pl.when(w == some)
                def _(some=some):
                    load(some, k).wait()

            acc[w] += lax.dot_general(x[j], gu[w, j], NT, preferred_element_type=f32)

        a = acc[0]
        out_ref[...] = ((acc[1] + 1.0) * a * jax.nn.sigmoid(1.702 * a)).astype(bf16)

    return kernel(
        body,
        (row, *pieces, gate_w, up_w),
        jax.ShapeDtypeStruct((h, units), bf16),
        [pltpu.VMEM((RING, h, WIDE), bf16)]
        + [pltpu.VMEM((2, *gate_w.shape), bf16)]
        + [pltpu.VMEM((2, h, units), f32)]
        + [pltpu.SemaphoreType.DMA((MANY, 2)), pltpu.SemaphoreType.DMA((2, RING))],
        9 * h // 512,
    )


def lower(row, hidden, down_w):
    h = hidden.shape[0]

    def body(row_ref, hid_ref, w_ref, *refs):
        outs = refs[:MANY]
        hid, d, y, hsem, wsem, ysem = refs[MANY:]
        row = row_ref[0]
        fetch = pltpu.make_async_copy(hid_ref, hid, hsem)
        fetch.start()

        def load(k):
            j = lax.rem(row + k, RING)
            return pltpu.make_async_copy(w_ref.at[j], d.at[j], wsem.at[k])

        for k in range(RING):
            load(RING - 1 - k).start()
        fetch.wait()

        @pl.loop(0, RING)
        def _(i):
            k = RING - 1 - i
            j = lax.rem(row + k, RING)
            load(k).wait()
            y[j] = jnp.dot(hid[...], d[j], preferred_element_type=f32).astype(bf16)
            for some in range(RING):

                @pl.when(k == some)
                def _(some=some):
                    for cp in copies(row, outs, GOES, y, ysem, True, some):
                        cp.start()

        for cp in copies(row, outs, GOES, y, ysem, True):
            cp.wait()

    return kernel(
        body,
        (row, hidden, down_w),
        [jax.ShapeDtypeStruct((len(k), h, LANES), bf16) for k in GOES],
        [pltpu.VMEM(hidden.shape, bf16), pltpu.VMEM(down_w.shape, bf16), pltpu.VMEM((RING, h, WIDE), bf16)]
        + [pltpu.SemaphoreType.DMA, pltpu.SemaphoreType.DMA((RING,)), pltpu.SemaphoreType.DMA((MANY, 2))],
        5 * h // 512,
    )


def shift(array, by):
    return lax.ppermute(array, "y", [(i, (i + by) % RING) for i in range(RING)])


def gathered(own):
    own = own.reshape(CORES, -1, LANES)
    a, b = own[:1], own[1:]
    back_a, fore_b = shift(a, 1), shift(b, -1)
    back_b, fore_a = shift(b, 1), shift(a, -1)
    far_a, far_b = shift(back_a, 1), shift(fore_b, -1)
    return own, back_a, fore_b, back_b, fore_a, far_a, far_b


def added(*parts):
    return sum(p.astype(f32) for p in parts).astype(bf16)


def scattered(parts):
    own, far_a, far_b, fore_b, back_a, later_a, later_b = parts
    far_a, far_b = shift(far_a, 1), shift(far_b, -1)
    fore_b, back_a = shift(fore_b, 1), shift(back_a, -1)
    later_a, later_b = shift(added(later_a, far_a), 1), shift(added(later_b, far_b), -1)
    total = jnp.concatenate([added(own[:1], back_a, later_a), added(own[1:], fore_b, later_b)])
    return total.reshape(-1, LANES)


def exchange(array):
    return lax.all_to_all(array, ("c", "x", "z"), 0, 0, tiled=True)


def local(tokens, expert_ids, combine_weights, gate_weight, up_weight, down_weight):
    experts = gate_weight.shape[0] * lax.axis_size(("x", "z"))
    feats = tokens.shape[1]
    core = lax.axis_index("c").astype(jnp.int32)
    row = lax.axis_index("y").astype(jnp.int32)[None]
    tok_t, ids_t, cw_t = tokens.T, expert_ids.T, combine_weights.T

    arranged = []
    for w in (gate_weight.swapaxes(1, 2), up_weight.swapaxes(1, 2), down_weight):
        other = lax.dynamic_index_in_dim(w, 1 - core, 0, keepdims=False)
        other = lax.ppermute(other, "c", [(0, 1), (1, 0)])
        arranged.append(arrange(core[None], w, other))

    returned, parts = [], []
    for i, size in enumerate(PARTS):
        start = sum(PARTS[:i])
        sent = dispatch(ids_t, tok_t, experts, start, size)
        sent = exchange(sent)
        pieces = gathered(sent)
        hidden = lift(row, pieces, *arranged[:2])
        part = lower(row, hidden, arranged[2])
        part = scattered(part)
        returned.append(exchange(part))
        parts.append(factors(ids_t, cw_t, experts, start, size))
    acc = None
    for i in range(len(PARTS)):
        acc = combine(returned[i], parts[i], acc, feats if i == len(PARTS) - 1 else None)
    return acc.T


def solution(mesh):
    split = Mesh(mesh.devices.reshape(4, -1, RING, CORES), ("x", "z", "y", "c"))
    ep, tp = ("x", "z"), ("y", "c")
    placed = (P(ep, tp), P(ep, None), P(ep, None), P(ep, None, tp), P(ep, None, tp), P(ep, tp, None))

    return jax.shard_map(local, mesh=split, in_specs=placed, out_specs=P(ep, tp), check_vma=False)
```

```python
import jax
import jax.numpy as jnp
from jax import lax
from jax.experimental import pallas as pl
from jax.experimental.pallas import tpu as pltpu
from jax.sharding import Mesh
from jax.sharding import PartitionSpec as P


PARTS = (16, 16)
CORES = 2
RING = 4
LANES = 384
HALF = 368
STEP = 112
GROUP = 32
WIDE = CORES * LANES
VMEM = 56 * 1024 * 1024

f32, bf16 = jnp.float32, jnp.bfloat16
NT = (((1,), (1,)), ((), ()))


def lasting(us):
    return pl.CostEstimate(flops=int(us * 250_000_000), bytes_accessed=0, transcendentals=0)


def slots_of(ids, experts):
    top, toks = ids.shape
    j = lax.broadcasted_iota(jnp.int32, (experts, toks), 0)
    chips = experts // CORES
    named = CORES * lax.rem(j, chips) + lax.div(j, chips)
    hit = [ids[k : k + 1, :] == named for k in range(top)]
    member = sum(h.astype(f32) for h in hit)
    before = lax.broadcasted_iota(jnp.int32, (toks, toks), 0) < lax.broadcasted_iota(jnp.int32, (toks, toks), 1)
    rank = jnp.dot(member.astype(bf16), before.astype(f32).astype(bf16), preferred_element_type=f32)
    return hit, jnp.where(member > 0, rank, -1.0)


def spread(rank, start, size):
    some, toks = rank.shape
    slot = lax.broadcasted_iota(jnp.int32, (some, size, toks), 1).astype(f32) + float(start)
    return jnp.broadcast_to(rank[:, None, :], (some, size, toks)) == slot


def dispatch(ids_t, tok_t, experts, start, size):
    feats, toks = tok_t.shape

    def body(ids_ref, tok_ref, out_ref, pad_ref, rank_ref):
        pad_ref[...] = jnp.zeros(pad_ref.shape, bf16)
        pad_ref[:feats, :] = tok_ref[...]
        rank_ref[...] = slots_of(ids_ref[...], experts)[1]

        @pl.loop(0, experts // GROUP)
        def _(i):
            rank = rank_ref[pl.ds(pl.multiple_of(i * GROUP, GROUP), GROUP), :]
            pick = spread(rank, start, size).astype(f32).reshape(GROUP * size, toks).astype(bf16)
            rows = lax.dot_general(pick, pad_ref[...], NT, preferred_element_type=f32)
            out_ref[pl.ds(pl.multiple_of(i * GROUP * size, GROUP * size), GROUP * size), :] = rows.astype(bf16)

    return pl.pallas_call(
        body,
        out_shape=jax.ShapeDtypeStruct((experts * size, LANES), bf16),
        scratch_shapes=[pltpu.VMEM((LANES, toks), bf16), pltpu.VMEM((experts, toks), f32)],
        compiler_params=pltpu.CompilerParams(vmem_limit_bytes=VMEM),
        cost_estimate=lasting(3),
    )(ids_t, tok_t)


def factors(ids_t, cw_t, experts, start, size):
    toks = ids_t.shape[1]

    def body(ids_ref, cw_ref, out_ref, rank_ref, weight_ref):
        hit, rank_ref[...] = slots_of(ids_ref[...], experts)
        cw = cw_ref[...]
        weight_ref[...] = sum(jnp.where(h, cw[k : k + 1, :], 0.0) for k, h in enumerate(hit))

        @pl.loop(0, experts // GROUP)
        def _(i):
            some = pl.ds(pl.multiple_of(i * GROUP, GROUP), GROUP)
            wide = jnp.broadcast_to(weight_ref[some, :][:, None, :], (GROUP, size, toks))
            coef = jnp.where(spread(rank_ref[some, :], start, size), wide, 0.0).reshape(GROUP * size, toks).T
            out_ref[:, pl.ds(pl.multiple_of(i * GROUP * size, GROUP * size), GROUP * size)] = coef.astype(bf16)

    return pl.pallas_call(
        body,
        out_shape=jax.ShapeDtypeStruct((toks, experts * size), bf16),
        scratch_shapes=[pltpu.VMEM((experts, toks), f32)] * 2,
        compiler_params=pltpu.CompilerParams(vmem_limit_bytes=VMEM),
        cost_estimate=lasting(4),
    )(ids_t, cw_t)


def combine(rows, factor):
    return lax.dot_general(rows, factor, (((0,), (1,)), ((), ())), preferred_element_type=f32)


def arrange(core, own, received):
    _, units, width = own.shape
    feats = width // (RING * CORES)

    def body(core_ref, own_ref, recv_ref, out_ref):
        for first in (0, HALF):
            out_ref[0, first + units : first + HALF, :] = jnp.zeros((HALF - units, WIDE), bf16)
        for c in range(CORES):
            out_ref[0, :, c * LANES + feats : (c + 1) * LANES] = jnp.zeros((2 * HALF, LANES - feats), bf16)
        for q in range(RING):

            @pl.when(pl.program_id(0) == q)
            def _(q=q):
                def move(at, size):
                    for c in range(CORES):
                        j = (CORES * q + c) * feats
                        to = slice(c * LANES, c * LANES + feats)
                        out_ref[0, pl.ds(at, size), to] = own_ref[0, pl.ds(at, size), j : j + feats]
                        out_ref[0, pl.ds(HALF + at, size), to] = recv_ref[pl.ds(at, size), j : j + feats]

                @pl.loop(0, units // STEP)
                def _(i):
                    move(pl.multiple_of(i * STEP, STEP), STEP)

                if units % STEP:
                    move(units - units % STEP, units % STEP)

    return pl.pallas_call(
        body,
        grid_spec=pltpu.PrefetchScalarGridSpec(
            num_scalar_prefetch=1,
            grid=(RING,),
            in_specs=[
                pl.BlockSpec((1, units, width), lambda i, c: (c[0], 0, 0)),
                pl.BlockSpec((units, width), lambda i, c: (0, 0)),
            ],
            out_specs=pl.BlockSpec((1, 2 * HALF, WIDE), lambda i, c: (i, 0, 0)),
        ),
        out_shape=jax.ShapeDtypeStruct((RING, 2 * HALF, WIDE), bf16),
        compiler_params=pltpu.CompilerParams(vmem_limit_bytes=VMEM),
        cost_estimate=lasting(6),
        name="arrange",
    )(core, own, received)


CAME = [((0, 0), (0, 1)), ((3, 0),), ((1, 1),), ((3, 1),), ((1, 0),), ((2, 0),), ((2, 1),)]
GOES = [((0, 0), (0, 1)), ((2, 0),), ((2, 1),), ((1, 1),), ((3, 0),), ((1, 0),), ((3, 1),)]
MANY = len(CAME)


def copies(row, arrays, keys, buf, sem, out, only=None):
    for i, (ref, blocks) in enumerate(zip(arrays, keys)):
        for b, (k, c) in enumerate(blocks):
            if only is None or only == k:
                here = buf.at[lax.rem(row + k, RING), :, pl.ds(c * LANES, LANES)]
                ends = (here, ref.at[b]) if out else (ref.at[b], here)
                yield pltpu.make_async_copy(*ends, sem.at[i, b])


def kernel(body, inputs, out_shape, scratch, us):
    hbm = pl.BlockSpec(memory_space=pltpu.MemorySpace.HBM)
    many = isinstance(out_shape, list)
    return pl.pallas_call(
        body,
        in_specs=[pl.BlockSpec(memory_space=pltpu.MemorySpace.SMEM)] + [hbm] * (len(inputs) - 1),
        out_specs=[hbm] * len(out_shape) if many else pl.BlockSpec(memory_space=pltpu.MemorySpace.VMEM),
        out_shape=out_shape,
        scratch_shapes=scratch,
        compiler_params=pltpu.CompilerParams(vmem_limit_bytes=VMEM),
        cost_estimate=lasting(us),
    )(*inputs)


def lift(row, pieces, gate_w, up_w):
    h = pieces[0].shape[1]
    units = gate_w.shape[1]

    def body(row_ref, *refs):
        xs, ws, out_ref = refs[:MANY], refs[MANY : MANY + 2], refs[MANY + 2]
        x, gu, acc, xsem, wsem = refs[MANY + 3 :]
        row = row_ref[0]

        def load(w, k):
            j = lax.rem(row + k, RING)
            return pltpu.make_async_copy(ws[w].at[j], gu.at[w, j], wsem.at[w, k])

        for k in range(RING):
            for cp in copies(row, xs, CAME, x, xsem, False, k):
                cp.start()
            load(0, k).start()
            load(1, k).start()
        acc[...] = jnp.zeros(acc.shape, f32)

        @pl.loop(0, 2 * RING)
        def _(i):
            k, w = lax.div(i, 2), lax.rem(i, 2)
            j = lax.rem(row + k, RING)
            for some in range(RING):

                @pl.when(i == 2 * some)
                def _(some=some):
                    for cp in copies(row, xs, CAME, x, xsem, False, some):
                        cp.wait()

            for some in range(2):

                @pl.when(w == some)
                def _(some=some):
                    load(some, k).wait()

            acc[w] += lax.dot_general(x[j], gu[w, j], NT, preferred_element_type=f32)

        a = acc[0]
        out_ref[...] = ((acc[1] + 1.0) * a * jax.nn.sigmoid(1.702 * a)).astype(bf16)

    return kernel(
        body,
        (row, *pieces, gate_w, up_w),
        jax.ShapeDtypeStruct((h, units), bf16),
        [pltpu.VMEM((RING, h, WIDE), bf16)]
        + [pltpu.VMEM((2, *gate_w.shape), bf16)]
        + [pltpu.VMEM((2, h, units), f32)]
        + [pltpu.SemaphoreType.DMA((MANY, 2)), pltpu.SemaphoreType.DMA((2, RING))],
        9 * h // 512,
    )


def lower(row, hidden, down_w):
    h = hidden.shape[0]

    def body(row_ref, hid_ref, w_ref, *refs):
        outs = refs[:MANY]
        hid, d, y, hsem, wsem, ysem = refs[MANY:]
        row = row_ref[0]
        fetch = pltpu.make_async_copy(hid_ref, hid, hsem)
        fetch.start()

        def load(k):
            j = lax.rem(row + k, RING)
            return pltpu.make_async_copy(w_ref.at[j], d.at[j], wsem.at[k])

        for k in range(RING):
            load(RING - 1 - k).start()
        fetch.wait()

        @pl.loop(0, RING)
        def _(i):
            k = RING - 1 - i
            j = lax.rem(row + k, RING)
            load(k).wait()
            y[j] = jnp.dot(hid[...], d[j], preferred_element_type=f32).astype(bf16)
            for some in range(RING):

                @pl.when(k == some)
                def _(some=some):
                    for cp in copies(row, outs, GOES, y, ysem, True, some):
                        cp.start()

        for cp in copies(row, outs, GOES, y, ysem, True):
            cp.wait()

    return kernel(
        body,
        (row, hidden, down_w),
        [jax.ShapeDtypeStruct((len(k), h, LANES), bf16) for k in GOES],
        [pltpu.VMEM(hidden.shape, bf16), pltpu.VMEM(down_w.shape, bf16), pltpu.VMEM((RING, h, WIDE), bf16)]
        + [pltpu.SemaphoreType.DMA, pltpu.SemaphoreType.DMA((RING,)), pltpu.SemaphoreType.DMA((MANY, 2))],
        5 * h // 512,
    )


def shift(array, by):
    return lax.ppermute(array, "y", [(i, (i + by) % RING) for i in range(RING)])


def gathered(own):
    own = own.reshape(CORES, -1, LANES)
    a, b = own[:1], own[1:]
    back_a, fore_b = shift(a, 1), shift(b, -1)
    back_b, fore_a = shift(b, 1), shift(a, -1)
    far_a, far_b = shift(back_a, 1), shift(fore_b, -1)
    return own, back_a, fore_b, back_b, fore_a, far_a, far_b


def added(*parts):
    return sum(p.astype(f32) for p in parts).astype(bf16)


def scattered(parts):
    own, far_a, far_b, fore_b, back_a, later_a, later_b = parts
    far_a, far_b = shift(far_a, 1), shift(far_b, -1)
    fore_b, back_a = shift(fore_b, 1), shift(back_a, -1)
    later_a, later_b = shift(added(later_a, far_a), 1), shift(added(later_b, far_b), -1)
    total = jnp.concatenate([added(own[:1], back_a, later_a), added(own[1:], fore_b, later_b)])
    return total.reshape(-1, LANES)


def exchange(array):
    return lax.all_to_all(array, ("c", "x", "z"), 0, 0, tiled=True)


def local(tokens, expert_ids, combine_weights, gate_weight, up_weight, down_weight):
    experts = gate_weight.shape[0] * lax.axis_size(("x", "z"))
    feats = tokens.shape[1]
    core = lax.axis_index("c").astype(jnp.int32)
    row = lax.axis_index("y").astype(jnp.int32)[None]
    tok_t, ids_t, cw_t = tokens.T, expert_ids.T, combine_weights.T

    arranged = []
    for w in (gate_weight.swapaxes(1, 2), up_weight.swapaxes(1, 2), down_weight):
        other = lax.dynamic_index_in_dim(w, 1 - core, 0, keepdims=False)
        other = lax.ppermute(other, "c", [(0, 1), (1, 0)])
        arranged.append(arrange(core[None], w, other))

    returned, parts = [], []
    for i, size in enumerate(PARTS):
        start = sum(PARTS[:i])
        sent = dispatch(ids_t, tok_t, experts, start, size)
        sent = exchange(sent)
        pieces = gathered(sent)
        hidden = lift(row, pieces, *arranged[:2])
        part = lower(row, hidden, arranged[2])
        part = scattered(part)
        returned.append(exchange(part))
        parts.append(factors(ids_t, cw_t, experts, start, size))
    total = 0.0
    for i in range(len(PARTS)):
        total += combine(returned[i], parts[i])
    return total[:feats].astype(bf16).T


def solution(mesh):
    split = Mesh(mesh.devices.reshape(4, -1, RING, CORES), ("x", "z", "y", "c"))
    ep, tp = ("x", "z"), ("y", "c")
    placed = (P(ep, tp), P(ep, None), P(ep, None), P(ep, None, tp), P(ep, None, tp), P(ep, tp, None))

    return jax.shard_map(local, mesh=split, in_specs=placed, out_specs=P(ep, tp), check_vma=False)
```

```python
import jax
import jax.numpy as jnp
from jax import lax
from jax.experimental import pallas as pl
from jax.experimental.pallas import tpu as pltpu
from jax.sharding import Mesh
from jax.sharding import PartitionSpec as P


PARTS = (16, 16)
CORES = 2
RING = 4
LANES = 384
HALF = 368
STEP = 112
GROUP = 32
WIDE = CORES * LANES
VMEM = 56 * 1024 * 1024

f32, bf16 = jnp.float32, jnp.bfloat16
NT = (((1,), (1,)), ((), ()))


def lasting(us):
    return pl.CostEstimate(flops=int(us * 250_000_000), bytes_accessed=0, transcendentals=0)


def slots_of(ids, experts):
    top, toks = ids.shape
    j = lax.broadcasted_iota(jnp.int32, (experts, toks), 0)
    chips = experts // CORES
    named = CORES * lax.rem(j, chips) + lax.div(j, chips)
    hit = [ids[k : k + 1, :] == named for k in range(top)]
    member = sum(h.astype(f32) for h in hit)
    before = lax.broadcasted_iota(jnp.int32, (toks, toks), 0) < lax.broadcasted_iota(jnp.int32, (toks, toks), 1)
    rank = jnp.dot(member.astype(bf16), before.astype(f32).astype(bf16), preferred_element_type=f32)
    return hit, jnp.where(member > 0, rank, -1.0)


def spread(rank, start, size):
    some, toks = rank.shape
    slot = lax.broadcasted_iota(jnp.int32, (some, size, toks), 1).astype(f32) + float(start)
    return jnp.broadcast_to(rank[:, None, :], (some, size, toks)) == slot


def dispatch(ids_t, tok_t, experts, start, size):
    feats, toks = tok_t.shape

    def body(ids_ref, tok_ref, out_ref, pad_ref):
        pad_ref[:feats, :] = tok_ref[...]
        pad_ref[feats:, :] = jnp.zeros((LANES - feats, toks), bf16)
        _, rank = slots_of(ids_ref[...], experts)
        pick = spread(rank, start, size).astype(f32).reshape(experts * size, toks).astype(bf16)
        out_ref[...] = lax.dot_general(pick, pad_ref[...], NT, preferred_element_type=f32).astype(bf16)

    return pl.pallas_call(
        body,
        out_shape=jax.ShapeDtypeStruct((experts * size, LANES), bf16),
        scratch_shapes=[pltpu.VMEM((LANES, toks), bf16)],
        compiler_params=pltpu.CompilerParams(vmem_limit_bytes=VMEM),
        cost_estimate=lasting(3),
    )(ids_t, tok_t)


def factors(ids_t, cw_t, experts, start, size):
    toks = ids_t.shape[1]

    def body(ids_ref, cw_ref, out_ref, rank_ref, weight_ref):
        hit, rank_ref[...] = slots_of(ids_ref[...], experts)
        cw = cw_ref[...]
        weight_ref[...] = sum(jnp.where(h, cw[k : k + 1, :], 0.0) for k, h in enumerate(hit))

        @pl.loop(0, experts // GROUP)
        def _(i):
            some = pl.ds(pl.multiple_of(i * GROUP, GROUP), GROUP)
            wide = jnp.broadcast_to(weight_ref[some, :][:, None, :], (GROUP, size, toks))
            coef = jnp.where(spread(rank_ref[some, :], start, size), wide, 0.0).reshape(GROUP * size, toks).T
            out_ref[:, pl.ds(pl.multiple_of(i * GROUP * size, GROUP * size), GROUP * size)] = coef.astype(bf16)

    return pl.pallas_call(
        body,
        out_shape=jax.ShapeDtypeStruct((toks, experts * size), bf16),
        scratch_shapes=[pltpu.VMEM((experts, toks), f32)] * 2,
        compiler_params=pltpu.CompilerParams(vmem_limit_bytes=VMEM),
        cost_estimate=lasting(4),
    )(ids_t, cw_t)


def combine(rows, factor):
    return lax.dot_general(rows, factor, (((0,), (1,)), ((), ())), preferred_element_type=f32)


def arrange(core, own, received):
    _, units, width = own.shape
    feats = width // (RING * CORES)

    def body(core_ref, own_ref, recv_ref, out_ref):
        for first in (0, HALF):
            out_ref[0, first + units : first + HALF, :] = jnp.zeros((HALF - units, WIDE), bf16)
        for c in range(CORES):
            out_ref[0, :, c * LANES + feats : (c + 1) * LANES] = jnp.zeros((2 * HALF, LANES - feats), bf16)
        for q in range(RING):

            @pl.when(pl.program_id(0) == q)
            def _(q=q):
                def move(at, size):
                    for c in range(CORES):
                        j = (CORES * q + c) * feats
                        to = slice(c * LANES, c * LANES + feats)
                        out_ref[0, pl.ds(at, size), to] = own_ref[0, pl.ds(at, size), j : j + feats]
                        out_ref[0, pl.ds(HALF + at, size), to] = recv_ref[pl.ds(at, size), j : j + feats]

                @pl.loop(0, units // STEP)
                def _(i):
                    move(pl.multiple_of(i * STEP, STEP), STEP)

                if units % STEP:
                    move(units - units % STEP, units % STEP)

    return pl.pallas_call(
        body,
        grid_spec=pltpu.PrefetchScalarGridSpec(
            num_scalar_prefetch=1,
            grid=(RING,),
            in_specs=[
                pl.BlockSpec((1, units, width), lambda i, c: (c[0], 0, 0)),
                pl.BlockSpec((units, width), lambda i, c: (0, 0)),
            ],
            out_specs=pl.BlockSpec((1, 2 * HALF, WIDE), lambda i, c: (i, 0, 0)),
        ),
        out_shape=jax.ShapeDtypeStruct((RING, 2 * HALF, WIDE), bf16),
        compiler_params=pltpu.CompilerParams(vmem_limit_bytes=VMEM),
        cost_estimate=lasting(6),
        name="arrange",
    )(core, own, received)


CAME = [((0, 0), (0, 1)), ((3, 0),), ((1, 1),), ((3, 1),), ((1, 0),), ((2, 0),), ((2, 1),)]
GOES = [((0, 0), (0, 1)), ((2, 0),), ((2, 1),), ((1, 1),), ((3, 0),), ((1, 0),), ((3, 1),)]
MANY = len(CAME)


def copies(row, arrays, keys, buf, sem, out, only=None):
    for i, (ref, blocks) in enumerate(zip(arrays, keys)):
        for b, (k, c) in enumerate(blocks):
            if only is None or only == k:
                here = buf.at[lax.rem(row + k, RING), :, pl.ds(c * LANES, LANES)]
                ends = (here, ref.at[b]) if out else (ref.at[b], here)
                yield pltpu.make_async_copy(*ends, sem.at[i, b])


def kernel(body, inputs, out_shape, scratch, us):
    hbm = pl.BlockSpec(memory_space=pltpu.MemorySpace.HBM)
    many = isinstance(out_shape, list)
    return pl.pallas_call(
        body,
        in_specs=[pl.BlockSpec(memory_space=pltpu.MemorySpace.SMEM)] + [hbm] * (len(inputs) - 1),
        out_specs=[hbm] * len(out_shape) if many else pl.BlockSpec(memory_space=pltpu.MemorySpace.VMEM),
        out_shape=out_shape,
        scratch_shapes=scratch,
        compiler_params=pltpu.CompilerParams(vmem_limit_bytes=VMEM),
        cost_estimate=lasting(us),
    )(*inputs)


def lift(row, pieces, gate_w, up_w):
    h = pieces[0].shape[1]
    units = gate_w.shape[1]

    def body(row_ref, *refs):
        xs, ws, out_ref = refs[:MANY], refs[MANY : MANY + 2], refs[MANY + 2]
        x, gu, acc, xsem, wsem = refs[MANY + 3 :]
        row = row_ref[0]

        def load(w, k):
            j = lax.rem(row + k, RING)
            return pltpu.make_async_copy(ws[w].at[j], gu.at[w, j], wsem.at[w, k])

        for k in range(RING):
            for cp in copies(row, xs, CAME, x, xsem, False, k):
                cp.start()
            load(0, k).start()
            load(1, k).start()
        acc[...] = jnp.zeros(acc.shape, f32)

        @pl.loop(0, 2 * RING)
        def _(i):
            k, w = lax.div(i, 2), lax.rem(i, 2)
            j = lax.rem(row + k, RING)
            for some in range(RING):

                @pl.when(i == 2 * some)
                def _(some=some):
                    for cp in copies(row, xs, CAME, x, xsem, False, some):
                        cp.wait()

            for some in range(2):

                @pl.when(w == some)
                def _(some=some):
                    load(some, k).wait()

            acc[w] += lax.dot_general(x[j], gu[w, j], NT, preferred_element_type=f32)

        a = acc[0]
        out_ref[...] = ((acc[1] + 1.0) * a * jax.nn.sigmoid(1.702 * a)).astype(bf16)

    return kernel(
        body,
        (row, *pieces, gate_w, up_w),
        jax.ShapeDtypeStruct((h, units), bf16),
        [pltpu.VMEM((RING, h, WIDE), bf16)]
        + [pltpu.VMEM((2, *gate_w.shape), bf16)]
        + [pltpu.VMEM((2, h, units), f32)]
        + [pltpu.SemaphoreType.DMA((MANY, 2)), pltpu.SemaphoreType.DMA((2, RING))],
        9 * h // 512,
    )


def lower(row, hidden, down_w):
    h = hidden.shape[0]

    def body(row_ref, hid_ref, w_ref, *refs):
        outs = refs[:MANY]
        hid, d, y, hsem, wsem, ysem = refs[MANY:]
        row = row_ref[0]
        fetch = pltpu.make_async_copy(hid_ref, hid, hsem)
        fetch.start()

        def load(k):
            j = lax.rem(row + k, RING)
            return pltpu.make_async_copy(w_ref.at[j], d.at[j], wsem.at[k])

        for k in range(RING):
            load(RING - 1 - k).start()
        fetch.wait()

        @pl.loop(0, RING)
        def _(i):
            k = RING - 1 - i
            j = lax.rem(row + k, RING)
            load(k).wait()
            y[j] = jnp.dot(hid[...], d[j], preferred_element_type=f32).astype(bf16)
            for some in range(RING):

                @pl.when(k == some)
                def _(some=some):
                    for cp in copies(row, outs, GOES, y, ysem, True, some):
                        cp.start()

        for cp in copies(row, outs, GOES, y, ysem, True):
            cp.wait()

    return kernel(
        body,
        (row, hidden, down_w),
        [jax.ShapeDtypeStruct((len(k), h, LANES), bf16) for k in GOES],
        [pltpu.VMEM(hidden.shape, bf16), pltpu.VMEM(down_w.shape, bf16), pltpu.VMEM((RING, h, WIDE), bf16)]
        + [pltpu.SemaphoreType.DMA, pltpu.SemaphoreType.DMA((RING,)), pltpu.SemaphoreType.DMA((MANY, 2))],
        5 * h // 512,
    )


def shift(array, by):
    return lax.ppermute(array, "y", [(i, (i + by) % RING) for i in range(RING)])


def gathered(own):
    own = own.reshape(CORES, -1, LANES)
    a, b = own[:1], own[1:]
    back_a, fore_b = shift(a, 1), shift(b, -1)
    back_b, fore_a = shift(b, 1), shift(a, -1)
    far_a, far_b = shift(back_a, 1), shift(fore_b, -1)
    return own, back_a, fore_b, back_b, fore_a, far_a, far_b


def added(*parts):
    return sum(p.astype(f32) for p in parts).astype(bf16)


def scattered(parts):
    own, far_a, far_b, fore_b, back_a, later_a, later_b = parts
    far_a, far_b = shift(far_a, 1), shift(far_b, -1)
    fore_b, back_a = shift(fore_b, 1), shift(back_a, -1)
    later_a, later_b = shift(added(later_a, far_a), 1), shift(added(later_b, far_b), -1)
    total = jnp.concatenate([added(own[:1], back_a, later_a), added(own[1:], fore_b, later_b)])
    return total.reshape(-1, LANES)


def exchange(array):
    return lax.all_to_all(array, ("c", "x", "z"), 0, 0, tiled=True)


def local(tokens, expert_ids, combine_weights, gate_weight, up_weight, down_weight):
    experts = gate_weight.shape[0] * lax.axis_size(("x", "z"))
    feats = tokens.shape[1]
    core = lax.axis_index("c").astype(jnp.int32)
    row = lax.axis_index("y").astype(jnp.int32)[None]
    tok_t, ids_t, cw_t = tokens.T, expert_ids.T, combine_weights.T

    arranged = []
    for w in (gate_weight.swapaxes(1, 2), up_weight.swapaxes(1, 2), down_weight):
        other = lax.dynamic_index_in_dim(w, 1 - core, 0, keepdims=False)
        other = lax.ppermute(other, "c", [(0, 1), (1, 0)])
        arranged.append(arrange(core[None], w, other))

    returned, parts = [], []
    for i, size in enumerate(PARTS):
        start = sum(PARTS[:i])
        sent = dispatch(ids_t, tok_t, experts, start, size)
        sent = exchange(sent)
        pieces = gathered(sent)
        hidden = lift(row, pieces, *arranged[:2])
        part = lower(row, hidden, arranged[2])
        part = scattered(part)
        returned.append(exchange(part))
        parts.append(factors(ids_t, cw_t, experts, start, size))
    total = 0.0
    for i in range(len(PARTS)):
        total += combine(returned[i], parts[i])
    return total[:feats].astype(bf16).T


def solution(mesh):
    split = Mesh(mesh.devices.reshape(4, -1, RING, CORES), ("x", "z", "y", "c"))
    ep, tp = ("x", "z"), ("y", "c")
    placed = (P(ep, tp), P(ep, None), P(ep, None), P(ep, None, tp), P(ep, None, tp), P(ep, tp, None))

    return jax.shard_map(local, mesh=split, in_specs=placed, out_specs=P(ep, tp), check_vma=False)
```
